32 devices in a mesh: gx: 4 (over z), gy: 8 (over y, x, core).
Axes of the slice: x: 2, y: 2, z: 4, core: 2. Of those that a mesh axis runs over, the one named last changes fastest.
Arguments:
- density: float32 [8, 512, 2048], P(None, 'gy', 'gx'), may hold values from -6 to 6
- tracer: float32 [8, 512, 2048], P(None, 'gy', 'gx'), may hold values from -6 to 6
- sea_mask: int32 [512, 2048], P('gy', 'gx'), may hold values 0 or 1
- mixed_level: int32 [512, 2048], P('gy', 'gx'), may hold values from 0 to 4
- tile_blocks: int32 [64], replicated, may hold values from 0 to 63, each once
- block_owner: int32 [64], replicated, may hold values from 0 to 63, as said below
Outputs:
- tracer_out: float32 [8, 512, 2048], P(None, 'gy', 'gx')
The draws below stay inside these ranges and needn't reach their ends.
Inputs may be any that keep to these rules, and one draw needn't show every extreme that they name: `sea_mask`: 1 marks sea, 0 land. `tile_blocks`: each of the 64 blocks once. `block_owner`: each of the 64 dynamics slots once; slot t belongs to gy index t // 8; of the 8 physics slots of one gy index, at most 2 go to any one gy index, and exactly 2 to every gy index that they reach.
All inputs are finite; a program needn't handle non-finite values. No bound on the sum of `sea_mask` on one device may be relied on, other than what follows from the above.
Results may differ from the reference program's by a relative error of at most 0.0003.
Values sent between devices are 32-bit elements; how exact they have to be, the bound alone decides.
A program may use at most 128 MiB of HBM per device.

```python
import jax
import jax.numpy as jnp
from jax import lax

K = 8
BR = 8
BPD = 8
CAP = 2
ITERS = 4
NBLK = 64
NY = 512
NX = 2048


def draw_block_owner(key, part):
    devices = NBLK // BPD
    key_offsets, key_order, key_shuffle, key_places = jax.random.split(key, 4)
    distinct = jax.random.permutation(key_offsets, devices)[:BPD // CAP]
    offsets = jax.random.permutation(key_order, jnp.repeat(distinct, CAP))
    shuffle = jax.random.permutation(key_shuffle, devices)
    places = jax.random.permutation(key_places, BPD)
    sources = jnp.arange(devices, dtype=jnp.int32)[:, None]
    targets = jnp.take(shuffle, (sources + offsets[None, :]) % devices)
    return (targets * BPD + places[None, :]).reshape(-1).astype(jnp.int32)


def set_ends(entries, own_key, low, high):
    longest = entries.shape.index(max(entries.shape))
    spots = []
    for shift in (0, 1):
        where = [jax.random.randint(jax.random.fold_in(own_key, axis), (), 0, length) for axis, length in enumerate(entries.shape)]
        where[longest] = (where[longest] + shift) % entries.shape[longest]
        spots.append(tuple(where))
    return entries.at[spots[0]].set(low).at[spots[1]].set(high)


def block_levels(stream_key, shape, pieces, smallest, high):
    level, own = 1.0, jax.random.fold_in(stream_key, 6)
    for axis_at, blocks in pieces:
        steps = jnp.exp(jax.random.uniform(jax.random.fold_in(own, axis_at), (blocks,), jnp.float32, smallest / len(pieces), high / len(pieces)))
        level = level * jnp.repeat(steps, shape[axis_at] // blocks).reshape([-1 if axis == axis_at else 1 for axis in range(len(shape))])
    return level


def noise(rng, shape, spread, most, shards=(), kind=jnp.bfloat16):
    values = jax.random.normal(rng, shape, jnp.float32) * spread
    if len(shards) > 0:
        values = block_levels(rng, shape, shards, -0.22, 0.18) * values
    return jnp.clip(values, min=-most, max=most).astype(kind)


def setup_inputs(seed: int = 0) -> dict:
    key_of = jax.random.split(jax.random.key(seed), 7)
    density = noise(key_of[0], (K, NY, NX), 1.0, 6.0, ((1, 8), (2, 4)), jnp.float32)
    tracer = noise(key_of[1], (K, NY, NX), 1.0, 6.0, ((1, 8), (2, 4)), jnp.float32)
    sea_mask = set_ends((jax.random.randint(key_of[2], (NY, NX), 0, 4) < 3).astype(jnp.int32), jax.random.fold_in(key_of[2], 1), 0, 1)
    mixed_level = set_ends(jax.random.randint(key_of[3], (NY, NX), 0, K // 2 + 1), jax.random.fold_in(key_of[3], 1), 0, (K // 2 + 1) - 1).astype(jnp.int32)
    tile_blocks = jax.random.permutation(key_of[4], NBLK).astype(jnp.int32)
    block_owner = draw_block_owner(jax.random.fold_in(key_of[6], 71), 0)
    return {"density": density, "tracer": tracer, "sea_mask": sea_mask, "mixed_level": mixed_level, "tile_blocks": tile_blocks, "block_owner": block_owner}


TIME_STEP = 0.2
STRATIFICATION = 1.0
DENSITY_FLOOR = 0.25
SLOPE_LIMIT = 1.0
TAPER_WIDTH = 0.5
KERNEL_OFFSET = 0.05
BASE_DIFFUSIVITY = 0.2
VISBECK_ALPHA = 0.5

def interior(quantity):
    return quantity[..., 1:-1, 1:-1]

def masked_steps(quantity, seawater):
    across_east = seawater[..., :, 1:] * seawater[..., :, :-1]
    across_north = seawater[..., 1:, :] * seawater[..., :-1, :]
    step_east = (quantity[..., :, 1:] - quantity[..., :, :-1]) * across_east
    step_north = (quantity[..., 1:, :] - quantity[..., :-1, :]) * across_north
    return (step_east, step_north)

def centered_east(step_east):
    return 0.5 * (step_east[..., 1:-1, 1:] + step_east[..., 1:-1, :-1])

def centered_north(step_north):
    return 0.5 * (step_north[..., 1:, 1:-1] + step_north[..., :-1, 1:-1])

def vertical_center(quantity):
    shallower = jnp.concatenate([quantity[:1], quantity[:-1]], axis=0)
    deeper = jnp.concatenate([quantity[1:], quantity[-1:]], axis=0)
    return 0.5 * (deeper - shallower)

def vertical_divergence(column_flux):
    zero_layer = jnp.zeros_like(column_flux[:1])
    shallower = jnp.concatenate([zero_layer, column_flux[:-1]], axis=0)
    deeper = jnp.concatenate([column_flux[1:], zero_layer], axis=0)
    return 0.5 * (deeper - shallower)

def physics(density_rim, seawater_rim, mixed_depth):
    level_count = density_rim.shape[0]
    levels = jnp.arange(level_count, dtype=jnp.float32).reshape(-1, 1, 1, 1)
    step_east, step_north = masked_steps(density_rim, seawater_rim)
    grad_east = centered_east(step_east)
    grad_north = centered_north(step_north)
    stratified = vertical_center(interior(density_rim) + STRATIFICATION * levels)
    denominator = jnp.maximum(stratified, DENSITY_FLOOR)
    slope_east = -grad_east / denominator
    slope_north = -grad_north / denominator
    squared = slope_east * slope_east + slope_north * slope_north
    taper_factor = 0.5 * (1.0 + jnp.tanh((SLOPE_LIMIT - squared) / TAPER_WIDTH))
    surface = jnp.minimum(1.0, (levels + 1.0) / (mixed_depth + 1.0))
    seawater = interior(seawater_rim)
    factor = taper_factor * surface * seawater
    slope_east = slope_east * factor
    slope_north = slope_north * factor
    tapered_sq = slope_east * slope_east + slope_north * slope_north
    below_layer = (levels >= mixed_depth).astype(jnp.float32)
    kernel = jnp.sqrt(denominator * (tapered_sq + KERNEL_OFFSET)) * below_layer
    depth_count = level_count - mixed_depth
    diffusivity = seawater * (BASE_DIFFUSIVITY + VISBECK_ALPHA * lax.optimization_barrier(jnp.sum(kernel, axis=0)) / depth_count)
    return (slope_east, slope_north, diffusivity)

def advance(tracer_rim, east_rim, north_rim, diffusivity_rim, seawater_rim):
    step_east, step_north = masked_steps(tracer_rim, seawater_rim)
    face_east = 0.5 * (diffusivity_rim[..., :, 1:] + diffusivity_rim[..., :, :-1]) * step_east
    face_north = 0.5 * (diffusivity_rim[..., 1:, :] + diffusivity_rim[..., :-1, :]) * step_north
    lateral = face_east[..., 1:-1, 1:] - face_east[..., 1:-1, :-1] + (face_north[..., 1:, 1:-1] - face_north[..., :-1, 1:-1])
    grad_east = centered_east(step_east)
    grad_north = centered_north(step_north)
    center_tracer = interior(tracer_rim)
    grad_down = vertical_center(center_tracer)
    slope_east = interior(east_rim)
    slope_north = interior(north_rim)
    column_flux = interior(diffusivity_rim) * (2.0 * slope_east * grad_east + 2.0 * slope_north * grad_north + (slope_east * slope_east + slope_north * slope_north) * grad_down)
    tendency = (lateral + vertical_divergence(column_flux)) * interior(seawater_rim)
    return center_tracer + TIME_STEP * tendency

def with_rim(quantity):
    leading = quantity.ndim - 2
    padded = jnp.pad(quantity, [(0, 0)] * leading + [(1, 1), (0, 0)])
    return jnp.pad(padded, [(0, 0)] * (leading + 1) + [(1, 1)], mode='wrap')

def reorder(quantity, ordering):
    leading = quantity.shape[:-2]
    blocks = quantity.reshape(leading + (ordering.shape[0], BR, quantity.shape[-1]))
    picked = jnp.take(blocks, ordering, axis=len(leading))
    return picked.reshape(quantity.shape)

def reference(density, tracer, sea_mask, mixed_level, tile_blocks, block_owner):
    physics_slot = jnp.argsort(tile_blocks).astype(jnp.int32)
    dynamics_blocks = jnp.take(tile_blocks, jnp.argsort(block_owner).astype(jnp.int32)).astype(jnp.int32)
    dynamics_slot = jnp.argsort(dynamics_blocks).astype(jnp.int32)
    density_grid = reorder(density, physics_slot)
    seawater = reorder(sea_mask, physics_slot).astype(jnp.float32)
    mixed_depth = reorder(mixed_level, physics_slot).astype(jnp.float32)
    seawater_rim = with_rim(seawater[None])
    slope_east, slope_north, diffusivity = physics(with_rim(density_grid[:, None]), seawater_rim, mixed_depth[None])
    diffusivity_rim = with_rim(diffusivity)
    east_rim = with_rim(slope_east)
    north_rim = with_rim(slope_north)
    current = reorder(tracer, dynamics_slot)[:, None]
    for sweep_index in range(ITERS):
        current = advance(with_rim(current), east_rim, north_rim, diffusivity_rim, seawater_rim)
    return reorder(current[:, 0], dynamics_blocks)
```

```python
import functools

import jax
import jax.numpy as jnp
from jax import lax
from jax.experimental import pallas as pl
from jax.experimental.pallas import tpu as pltpu
from jax.sharding import PartitionSpec as P

BR = 8
BPD = 8
ITERS = 4
EDGE = 8
LANES = 128
EROWS = 16

TIME_STEP = 0.2
STRATIFICATION = 1.0
DENSITY_FLOOR = 0.25
SLOPE_LIMIT = 1.0
TAPER_WIDTH = 0.5
KERNEL_OFFSET = 0.05
BASE_DIFFUSIVITY = 0.2
VISBECK_ALPHA = 0.5

MESH = pl.DeviceIdType.MESH


def pack_kernel(levels, dl, dr, tl, tr, ml, mr, xl, xr, left_ref, right_ref):
    lane = lax.broadcasted_iota(jnp.int32, (BR, LANES), 1)
    row = lax.broadcasted_iota(jnp.int32, (BR, LANES), 0)

    def one(tile, shift, keep):
        tile = jnp.where(keep, tile, 0.0)
        tile = pltpu.roll(tile, (shift + (BR - 1) * EDGE) % LANES, 1)
        for bit in (1, 2, 4):
            tile = jnp.where((row & bit) > 0, pltpu.roll(tile, LANES - bit * EDGE, 1), tile)
        return jnp.sum(tile, axis=0, keepdims=True)

    def side(b, d, t, m, x, out_ref, base, keep):
        tiles = [d[k, b] for k in range(levels)]
        tiles += [m[b].astype(jnp.float32), x[b].astype(jnp.float32)]
        tiles += [t[k, b] for k in range(levels)]
        half = LANES // 2
        rows = [
            one(tiles[2 * j], base, keep) + one(tiles[2 * j + 1], base + half, keep)
            for j in range(levels + 1)
        ]
        rows.append(jnp.zeros((EROWS - levels - 1, LANES), jnp.float32))
        out_ref[b] = jnp.concatenate(rows, axis=0)

    @pl.loop(0, BPD)
    def _(b):
        side(b, dl, tl, ml, xl, left_ref, 0, lane < EDGE)
        side(b, dr, tr, mr, xr, right_ref, EDGE, lane >= LANES - EDGE)


def pack_edges(density, tracer, sea, mixed):
    levels = density.shape[0]
    last = density.shape[-1] // LANES - 1
    big = lambda at: pl.BlockSpec((levels, BPD, BR, LANES), lambda i: (0, 0, 0, at))
    flat = lambda at: pl.BlockSpec((BPD, BR, LANES), lambda i: (0, 0, at))
    whole = pl.BlockSpec((BPD, EROWS, LANES), lambda i: (0, 0, 0))
    shape = jax.ShapeDtypeStruct((BPD, EROWS, LANES), jnp.float32)
    return pl.pallas_call(
        functools.partial(pack_kernel, levels),
        grid=(1,),
        in_specs=[big(0), big(last), big(0), big(last), flat(0), flat(last), flat(0), flat(last)],
        out_specs=[whole, whole],
        out_shape=[shape, shape],
        name="pack_edges",
    )(density, density, tracer, tracer, sea, sea, mixed, mixed)


def gather_kernel(
    columns, d, m, x, t, left, right,
    gd, gm, gx, gt, gel, ger,
    vd, vm, vx, vt, in_sem, own_sem, z_send, z_recv, send_sem, recv_sem,
):
    me = lax.axis_index("gy")
    mx = lax.axis_index("gx")
    east = lax.rem(mx + 1, columns)
    west = lax.rem(mx + columns - 1, columns)

    def flip(bit):
        return me + bit - 2 * bit * lax.rem(me // bit, 2)

    core, ex, wy = flip(1), flip(2), flip(4)
    diag = flip(2) + flip(4) - me
    offset_core = core - me
    barrier = pltpu.get_barrier_semaphore()
    for peer in (core, ex, wy):
        pl.semaphore_signal(barrier, inc=1, device_id={"gy": peer}, device_id_type=MESH)
    for peer in (east, west):
        pl.semaphore_signal(barrier, inc=1, device_id={"gx": peer}, device_id_type=MESH)
    pl.semaphore_wait(barrier, 5)

    low = d.shape[0] // 2
    cut = lambda ref, h: ref.at[pl.ds(h * low, low)]
    part = lambda ref, h: (lambda slot: ref.at[slot, pl.ds(h * low, low)])
    whole = lambda ref: (lambda slot: ref.at[slot])
    pieces = [
        (cut(d, 0), cut(vd, 0), part(gd, 0), 0),
        (cut(d, 1), cut(vd, 1), part(gd, 1), 1),
        (m, vm, whole(gm), 0),
        (x, vx, whole(gx), 1),
        (cut(t, 0), cut(vt, 0), part(gt, 0), 0),
        (cut(t, 1), cut(vt, 1), part(gt, 1), 1),
        (None, None, whole(gel), 0),
        (None, None, whole(ger), 1),
    ]
    staged = {}
    for i, (src, dst, _, _) in enumerate(pieces):
        if src is not None:
            staged[i] = pltpu.make_async_copy(src, dst, in_sem.at[i])
            staged[i].start()
    z_copies = [
        pltpu.make_async_remote_copy(
            right, gel.at[me], z_send.at[0], z_recv.at[0],
            device_id={"gx": east}, device_id_type=MESH),
        pltpu.make_async_remote_copy(
            left, ger.at[me], z_send.at[1], z_recv.at[1],
            device_id={"gx": west}, device_id_type=MESH),
    ]
    for copy in z_copies:
        copy.start()

    sent = {}

    def send(i, kind, src, slot, peer):
        copy = pltpu.make_async_remote_copy(
            src, pieces[i][2](slot), send_sem.at[i, kind], recv_sem.at[i, kind],
            device_id={"gy": peer}, device_id_type=MESH)
        copy.start()
        sent[i, kind] = copy

    own = []
    for i, (src, stage, place, _) in enumerate(pieces):
        if src is None:
            z_copies[i - len(staged)].wait_recv()
            stage = place(me)
        else:
            staged[i].wait()
        send(i, 0, stage, me, ex)
        send(i, 1, stage, me, wy)
        send(i, 2, stage, me, core)
        if src is not None:
            keep = pltpu.make_async_copy(stage, place(me), own_sem.at[i])
            keep.start()
            own.append(keep)
    for i, (_, _, place, way) in enumerate(pieces):
        sent[i, 0].wait_recv()
        if way == 0:
            send(i, 3, place(ex), ex, wy)
        send(i, 4, place(ex), ex, core)
        sent[i, 1].wait_recv()
        if way == 1:
            send(i, 3, place(wy), wy, ex)
        send(i, 5, place(wy), wy, core)
    for i, (_, _, place, _) in enumerate(pieces):
        sent[i, 3].wait_recv()
        send(i, 6, place(diag), diag, core)
    for i in range(len(pieces)):
        for kind in (2, 4, 5, 6):
            sent[i, kind].wait_recv()
    for copy in sent.values():
        copy.wait_send()
    for copy in z_copies:
        copy.wait_send()
    for copy in own:
        copy.wait()


def gather_blocks(count, columns, density, sea, mixed, tracer, left, right):
    arrays = (density, sea, mixed, tracer, left, right)
    if count != 8:
        ring = [(i, (i + 1) % columns) for i in range(columns)]
        back = [((i + 1) % columns, i) for i in range(columns)]
        arrays = arrays[:4] + (lax.ppermute(right, "gx", ring), lax.ppermute(left, "gx", back))
        return tuple(lax.all_gather(a, "gy", axis=0) for a in arrays)
    hbm = pl.BlockSpec(memory_space=pl.ANY)
    dma = pltpu.SemaphoreType.DMA
    return pl.pallas_call(
        functools.partial(gather_kernel, columns),
        in_specs=[hbm] * 6,
        out_specs=[hbm] * 6,
        out_shape=[jax.ShapeDtypeStruct((count,) + a.shape, a.dtype) for a in arrays],
        scratch_shapes=[pltpu.VMEM(a.shape, a.dtype) for a in arrays[:4]]
        + [dma((8,)), dma((8,)), dma((2,)), dma((2,)), dma((8, 7)), dma((8, 7))],
        compiler_params=pltpu.CompilerParams(collective_id=0, has_side_effects=True),
        name="gather_blocks",
    )(*arrays)


def block_kernel(levels, width, slots, dslots, valid, *refs):
    d, m, x, t = refs[0:3], refs[3:6], refs[6:9], refs[9:12]
    pel, per, tel, ter = refs[12:15], refs[15:18], refs[18:21], refs[21:24]
    out, grid_ref, cur, ae_ref, an_ref, av_ref, col = refs[24:]
    j = pl.program_id(0)
    wide = width + LANES
    rows = 2 * BR
    rim = BR // 2
    lane = lax.broadcasted_iota(jnp.int32, (BR, LANES), 1)

    def edge_tile(l_ref, r_ref, ch):
        row, base = ch // 2, (ch % 2) * (LANES // 2)

        def spread(ref, to):
            line = jnp.broadcast_to(ref[0, 0, row : row + 1, :], (BR, LANES))
            shift = (to - base - (BR - 1) * EDGE) % LANES
            return pltpu.roll(line, shift, 1, stride=EDGE, stride_axis=0)

        return jnp.where(
            lane < EDGE,
            spread(r_ref, 0),
            jnp.where(lane >= LANES - EDGE, spread(l_ref, LANES - EDGE), 0.0),
        )

    for o in range(3):
        here = pl.ds(o * BR, BR)
        there = valid[3 * j + o].astype(jnp.float32)
        for k in range(levels):
            grid_ref[k, here, :width] = d[o][0, k, 0]
            grid_ref[k, here, width:] = edge_tile(pel[o], per[o], k)
        grid_ref[levels, here, :width] = m[o][0, 0].astype(jnp.float32) * there
        grid_ref[levels, here, width:] = edge_tile(pel[o], per[o], levels) * there
        grid_ref[levels + 1, here, :width] = x[o][0, 0].astype(jnp.float32)
        grid_ref[levels + 1, here, width:] = edge_tile(pel[o], per[o], levels + 1)
        first, size, at = ((rim, rim, 0), (0, BR, rim), (0, rim, rim + BR))[o]
        for k in range(levels):
            cur[k, at : at + size, :width] = t[o][0, k, 0, first : first + size, :]
            tile = edge_tile(tel[o], ter[o], levels + 2 + k)
            cur[k, at : at + size, width:] = tile[first : first + size]

    east = lambda f: pltpu.roll(f, wide - 1, 1)
    west = lambda f: pltpu.roll(f, 1, 1)
    north = lambda f: pltpu.roll(f, rows - 1, 0)
    south = lambda f: pltpu.roll(f, 1, 0)
    mid = lambda k: grid_ref[k, rim : rim + rows, :]
    up = lambda k: grid_ref[k, rim + 1 : rim + 1 + rows, :]
    down = lambda k: grid_ref[k, rim - 1 : rim - 1 + rows, :]

    sea = mid(levels)
    col[0] = sea * east(sea)
    col[1] = sea * west(sea)
    col[2] = sea * up(levels)
    col[3] = sea * down(levels)
    depth = mid(levels + 1)
    col[4] = 1.0 / (depth + 1.0)
    total = jnp.zeros((rows, wide), jnp.float32)
    for k in range(levels):
        c = mid(k)
        ge = 0.5 * ((east(c) - c) * col[0] + (c - west(c)) * col[1])
        gn = 0.5 * ((up(k) - c) * col[2] + (c - down(k)) * col[3])
        hi, lo = min(k + 1, levels - 1), max(k - 1, 0)
        den = jnp.maximum(
            0.5 * (mid(hi) - mid(lo)) + 0.5 * STRATIFICATION * (hi - lo), DENSITY_FLOOR)
        inv = 1.0 / den
        se = -ge * inv
        sn = -gn * inv
        q = se * se + sn * sn
        taper = 0.5 * (1.0 + jnp.tanh((SLOPE_LIMIT - q) * (1.0 / TAPER_WIDTH)))
        factor = taper * jnp.minimum(1.0, (k + 1.0) * col[4]) * mid(levels)
        se = se * factor
        sn = sn * factor
        sq = se * se + sn * sn
        ae_ref[k] = se
        an_ref[k] = sn
        av_ref[k] = sq
        kern = jnp.sqrt(den * (sq + KERNEL_OFFSET))
        total = total + jnp.where(mid(levels + 1) <= k, kern, 0.0)
    sea = mid(levels)
    diff = sea * (
        BASE_DIFFUSIVITY + VISBECK_ALPHA * total / (levels - mid(levels + 1)))
    for k in range(levels):
        ae_ref[k] = ae_ref[k] * diff
        an_ref[k] = an_ref[k] * diff
        av_ref[k] = av_ref[k] * (0.5 * diff)
    step = (0.5 * TIME_STEP) * sea
    col[4] = (diff + east(diff)) * step * col[0]
    col[5] = (diff + west(diff)) * step * col[1]
    col[6] = (diff + north(diff)) * step * col[2]
    col[7] = (diff + south(diff)) * step * col[3]
    col[8] = step

    def iterate(_, carry):
        before = None
        flux = None
        held = None
        for k in range(levels):
            c = cur[k]
            de = east(c) - c
            dw = west(de)
            dn = north(c) - c
            ds = south(dn)
            dv = cur[min(k + 1, levels - 1)] - cur[max(k - 1, 0)]
            f = (
                ae_ref[k] * (col[0] * de + col[1] * dw)
                + an_ref[k] * (col[2] * dn + col[3] * ds)
                + av_ref[k] * dv
            )
            u = c + ((col[4] * de - col[5] * dw) + (col[6] * dn - col[7] * ds))
            if k > 0:
                jump = f if before is None else f - before
                cur[k - 1] = held + col[8] * jump
            before, flux, held = flux, f, u
        cur[levels - 1] = held - col[8] * before
        return carry

    lax.fori_loop(0, ITERS, iterate, 0)
    for k in range(levels):
        out[k, 0] = cur[k, rim : rim + BR, :width]


def run_blocks(slots, dslots, valid, gd, gm, gx, gt, gel, ger):
    levels, width = gd.shape[1], gd.shape[-1]

    def five(which, o):
        def at(j, *pre):
            s = pre[which][3 * j + o]
            return (lax.div(s, BPD), 0, lax.rem(s, BPD), 0, 0)
        return pl.BlockSpec((1, levels, 1, BR, width), at)

    def four(which, o, shape):
        def at(j, *pre):
            s = pre[which][3 * j + o]
            return (lax.div(s, BPD), lax.rem(s, BPD), 0, 0)
        return pl.BlockSpec((1, 1) + shape, at)

    three = range(3)
    edges = (EROWS, LANES)
    specs = [five(0, o) for o in three]
    specs += [four(0, o, (BR, width)) for o in three] * 2
    specs += [five(1, o) for o in three]
    specs += [four(0, o, edges) for o in three] * 2
    specs += [four(1, o, edges) for o in three] * 2
    wide = width + LANES
    f32 = lambda *shape: pltpu.VMEM(shape, jnp.float32)
    return pl.pallas_call(
        functools.partial(block_kernel, levels, width),
        grid_spec=pltpu.PrefetchScalarGridSpec(
            num_scalar_prefetch=3,
            grid=(BPD,),
            in_specs=specs,
            out_specs=pl.BlockSpec((levels, 1, BR, width), lambda j, *pre: (0, j, 0, 0)),
            scratch_shapes=[
                f32(levels + 2, 3 * BR, wide),
                f32(levels, 2 * BR, wide),
                f32(levels, 2 * BR, wide),
                f32(levels, 2 * BR, wide),
                f32(levels, 2 * BR, wide),
                f32(9, 2 * BR, wide),
            ],
        ),
        out_shape=jax.ShapeDtypeStruct((levels, BPD, BR, width), jnp.float32),
        name="run_blocks",
    )(
        slots, dslots, valid,
        gd, gd, gd, gm, gm, gm, gx, gx, gx, gt, gt, gt,
        gel, gel, gel, ger, ger, ger, gel, gel, gel, ger, ger, ger,
    )


def plan(tile_blocks, block_owner):
    blocks = tile_blocks.shape[0]
    at = jnp.arange(blocks, dtype=jnp.int32)
    mine = lax.axis_index("gy") * BPD + jnp.arange(BPD, dtype=jnp.int32)
    ids = jnp.sum(jnp.where(block_owner[None] == mine[:, None], tile_blocks[None], 0), axis=1)
    near = ids[:, None] + jnp.arange(-1, 2, dtype=jnp.int32)[None]
    valid = ((near >= 0) & (near < blocks)).astype(jnp.int32)
    near = jnp.clip(near, 0, blocks - 1)
    hit = tile_blocks[None, None] == near[..., None]
    slots = jnp.sum(jnp.where(hit, at, 0), axis=-1)
    dslots = jnp.sum(jnp.where(hit, block_owner, 0), axis=-1)
    return slots.reshape(-1), dslots.reshape(-1), valid.reshape(-1)


def on_device(count, columns, density, tracer, sea_mask, mixed_level, tile_blocks, block_owner):
    levels, height, width = density.shape
    split = lambda a: a.reshape(a.shape[:-2] + (BPD, BR, width))
    slots, dslots, valid = plan(tile_blocks, block_owner)
    density, tracer, sea, mixed = map(split, (density, tracer, sea_mask, mixed_level))
    left, right = pack_edges(density, tracer, sea, mixed)
    gathered = gather_blocks(count, columns, density, sea, mixed, tracer, left, right)
    gd, gm, gx, gt, gel, ger = gathered
    out = run_blocks(slots, dslots, valid, gd, gm, gx, gt, gel, ger)
    return out.reshape(levels, height, width)


def solution(mesh):
    placed = (P(None, "gy", "gx"), P(None, "gy", "gx"), P("gy", "gx"), P("gy", "gx"), P(), P())
    return jax.shard_map(
        functools.partial(on_device, mesh.shape["gy"], mesh.shape["gx"]),
        mesh=mesh, in_specs=placed, out_specs=P(None, "gy", "gx"), check_vma=False,
    )
```

```python
import functools

import jax
import jax.numpy as jnp
from jax import lax
from jax.experimental import pallas as pl
from jax.experimental.pallas import tpu as pltpu
from jax.sharding import PartitionSpec as P

BR = 8
BPD = 8
ITERS = 4
EDGE = 8
LANES = 128

TIME_STEP = 0.2
STRATIFICATION = 1.0
DENSITY_FLOOR = 0.25
SLOPE_LIMIT = 1.0
TAPER_WIDTH = 0.5
KERNEL_OFFSET = 0.05
BASE_DIFFUSIVITY = 0.2
VISBECK_ALPHA = 0.5

MESH = pl.DeviceIdType.MESH


def own_lane():
    return lax.broadcasted_iota(jnp.int32, (BR, LANES), 1)


def pack_edges(levels, d, m, x, t, left_ref, right_ref):
    lane = own_lane()
    row = lax.broadcasted_iota(jnp.int32, (BR, LANES), 0)
    end = d.shape[-1] - LANES

    def one(tile, shift, keep):
        tile = jnp.where(keep, tile, 0.0)
        tile = pltpu.roll(tile, (shift + (BR - 1) * EDGE) % LANES, 1)
        for bit in (1, 2, 4):
            tile = jnp.where((row & bit) > 0, pltpu.roll(tile, LANES - bit * EDGE, 1), tile)
        return jnp.sum(tile, axis=0, keepdims=True)

    def side(b, start, out_ref, base, keep):
        span = pl.ds(start, LANES)
        tiles = [d[k, b, :, span] for k in range(levels)]
        tiles += [m[b, :, span].astype(jnp.float32), x[b, :, span].astype(jnp.float32)]
        tiles += [t[k, b, :, span] for k in range(levels)]
        half = LANES // 2
        for j in range(levels + 1):
            out_ref[j, pl.ds(b, 1), :] = (
                one(tiles[2 * j], base, keep) + one(tiles[2 * j + 1], base + half, keep))

    def step(b, carry):
        side(b, 0, left_ref, 0, lane < EDGE)
        side(b, end, right_ref, EDGE, lane >= LANES - EDGE)
        return carry

    lax.fori_loop(0, BPD, step, 0)


def edge_tile(lane, l_row, r_row, ch):
    base = (ch % 2) * (LANES // 2)

    def spread(row, to):
        line = jnp.broadcast_to(row(ch // 2), (BR, LANES))
        shift = (to - base - (BR - 1) * EDGE) % LANES
        return pltpu.roll(line, shift, 1, stride=EDGE, stride_axis=0)

    return jnp.where(
        lane < EDGE,
        spread(r_row, 0),
        jnp.where(lane >= LANES - EDGE, spread(l_row, LANES - EDGE), 0.0),
    )


def shifts(rows, wide):
    east = lambda f: pltpu.roll(f, wide - 1, 1)
    west = lambda f: pltpu.roll(f, 1, 1)
    north = lambda f: pltpu.roll(f, rows - 1, 0)
    south = lambda f: pltpu.roll(f, 1, 0)
    return east, west, north, south


def physics_block(levels, width, get, l_row, r_row, there, grid_ref, ae_ref, an_ref, av_ref, col):
    wide = width + LANES
    rows = 2 * BR
    rim = BR // 2
    lane = own_lane()
    for o in range(3):
        here = pl.ds(o * BR, BR)
        for k in range(levels + 2):
            main = get(o, k)
            tile = edge_tile(lane, l_row(o), r_row(o), k)
            if k == levels:
                main, tile = main * there[o], tile * there[o]
            grid_ref[k, here, :width] = main
            grid_ref[k, here, width:] = tile

    east, west, north, south = shifts(rows, wide)
    mid = lambda k: grid_ref[k, rim : rim + rows, :]
    up = lambda k: grid_ref[k, rim + 1 : rim + 1 + rows, :]
    down = lambda k: grid_ref[k, rim - 1 : rim - 1 + rows, :]

    sea = mid(levels)
    col[0] = sea * east(sea)
    col[1] = sea * west(sea)
    col[2] = sea * up(levels)
    col[3] = sea * down(levels)
    depth = mid(levels + 1)
    col[4] = 1.0 / (depth + 1.0)
    total = jnp.zeros((rows, wide), jnp.float32)
    for k in range(levels):
        c = mid(k)
        ge = 0.5 * ((east(c) - c) * col[0] + (c - west(c)) * col[1])
        gn = 0.5 * ((up(k) - c) * col[2] + (c - down(k)) * col[3])
        hi, lo = min(k + 1, levels - 1), max(k - 1, 0)
        den = jnp.maximum(
            0.5 * (mid(hi) - mid(lo)) + 0.5 * STRATIFICATION * (hi - lo), DENSITY_FLOOR)
        inv = 1.0 / den
        se = -ge * inv
        sn = -gn * inv
        q = se * se + sn * sn
        taper = 0.5 * (1.0 + jnp.tanh((SLOPE_LIMIT - q) * (1.0 / TAPER_WIDTH)))
        factor = taper * jnp.minimum(1.0, (k + 1.0) * col[4]) * mid(levels)
        se = se * factor
        sn = sn * factor
        sq = se * se + sn * sn
        ae_ref[k] = se
        an_ref[k] = sn
        av_ref[k] = sq
        kern = jnp.sqrt(den * (sq + KERNEL_OFFSET))
        total = total + jnp.where(mid(levels + 1) <= k, kern, 0.0)
    sea = mid(levels)
    diff = sea * (
        BASE_DIFFUSIVITY + VISBECK_ALPHA * total / (levels - mid(levels + 1)))
    for k in range(levels):
        ae_ref[k] = ae_ref[k] * diff
        an_ref[k] = an_ref[k] * diff
        av_ref[k] = av_ref[k] * (0.5 * diff)
    step = (0.5 * TIME_STEP) * sea
    col[4] = (diff + east(diff)) * step * col[0]
    col[5] = (diff + west(diff)) * step * col[1]
    col[6] = (diff + north(diff)) * step * col[2]
    col[7] = (diff + south(diff)) * step * col[3]
    col[8] = step


def advance_block(levels, width, get, l_row, r_row, cur, ae_ref, an_ref, av_ref, col, put):
    wide = width + LANES
    rows = 2 * BR
    rim = BR // 2
    lane = own_lane()
    for o in range(3):
        first, size, at = ((rim, rim, 0), (0, BR, rim), (0, rim, rim + BR))[o]
        for k in range(levels):
            cur[k, at : at + size, :width] = get(o, k)[first : first + size]
            tile = edge_tile(lane, l_row(o), r_row(o), levels + 2 + k)
            cur[k, at : at + size, width:] = tile[first : first + size]
    east, west, north, south = shifts(rows, wide)

    def iterate(_, carry):
        before = None
        flux = None
        held = None
        for k in range(levels):
            c = cur[k]
            de = east(c) - c
            dw = west(de)
            dn = north(c) - c
            ds = south(dn)
            dv = cur[min(k + 1, levels - 1)] - cur[max(k - 1, 0)]
            f = (
                ae_ref[k] * (col[0] * de + col[1] * dw)
                + an_ref[k] * (col[2] * dn + col[3] * ds)
                + av_ref[k] * dv
            )
            u = c + ((col[4] * de - col[5] * dw) + (col[6] * dn - col[7] * ds))
            if k > 0:
                jump = f if before is None else f - before
                cur[k - 1] = held + col[8] * jump
            before, flux, held = flux, f, u
        cur[levels - 1] = held - col[8] * before
        return carry

    lax.fori_loop(0, ITERS, iterate, 0)
    for k in range(levels):
        put(k, cur[k, rim : rim + BR, :width])


def gathered_block(levels, blocks, codes, j, gd, gm, gx, gt, gel, ger):
    code = [codes[3 * j + o] for o in range(3)]
    pair = [lax.rem(c, blocks * blocks) for c in code]
    there = [lax.div(c, blocks * blocks).astype(jnp.float32) for c in code]

    def where(slot):
        return lax.div(slot, BPD), lax.rem(slot, BPD)

    phys = [where(lax.rem(p, blocks)) for p in pair]
    dyn = [where(lax.div(p, blocks)) for p in pair]

    def grid(o, k):
        dev, at = phys[o]
        if k < levels:
            return gd[dev, k, at]
        return (gm if k == levels else gx)[dev, at].astype(jnp.float32)

    def tracer(o, k):
        dev, at = dyn[o]
        return gt[dev, k, at]

    def row_of(ref, places):
        return lambda o: (lambda r: ref[places[o][0], r, pl.ds(places[o][1], 1), :])

    rows = [row_of(ref, places) for places in (phys, dyn) for ref in (gel, ger)]
    return there, grid, tracer, rows


def whole_kernel(
    columns, codes, d, m, x, t, out,
    gd, gm, gx, gt, gel, ger, left, right,
    grid_ref, cur, ae, an, av, col,
    in_sem, z_send, z_recv, send_sem, recv_sem,
):
    levels, width = d.shape[0], d.shape[-1]
    count = gd.shape[0]
    blocks = count * BPD
    me = lax.axis_index("gy")
    mx = lax.axis_index("gx")
    east = lax.rem(mx + 1, columns)
    west = lax.rem(mx + columns - 1, columns)

    def flip(bit):
        return me + bit - 2 * bit * lax.rem(me // bit, 2)

    core, ex, wy = flip(1), flip(2), flip(4)
    diag = flip(2) + flip(4) - me
    low = levels // 2
    cut = lambda ref, h: ref.at[pl.ds(h * low, low)]
    part = lambda ref, h: (lambda slot: ref.at[slot, pl.ds(h * low, low)])
    whole = lambda ref: (lambda slot: ref.at[slot])
    pieces = [
        (cut(d, 0), part(gd, 0), 0),
        (cut(d, 1), part(gd, 1), 1),
        (m, whole(gm), 0),
        (x, whole(gx), 1),
        (None, whole(gel), 0),
        (None, whole(ger), 1),
        (cut(t, 0), part(gt, 0), 0),
        (cut(t, 1), part(gt, 1), 1),
    ]
    staged = {}
    for i, (src, place, _) in enumerate(pieces):
        if src is not None:
            staged[i] = pltpu.make_async_copy(src, place(me), in_sem.at[i])
            staged[i].start()

    barrier = pltpu.get_barrier_semaphore()
    for peer in (core, ex, wy):
        pl.semaphore_signal(barrier, inc=1, device_id={"gy": peer}, device_id_type=MESH)
    for peer in (east, west):
        pl.semaphore_signal(barrier, inc=1, device_id={"gx": peer}, device_id_type=MESH)
    pl.semaphore_wait(barrier, 5)

    z_copies = [
        pltpu.make_async_remote_copy(
            right, gel.at[me], z_send.at[0], z_recv.at[0],
            device_id={"gx": east}, device_id_type=MESH),
        pltpu.make_async_remote_copy(
            left, ger.at[me], z_send.at[1], z_recv.at[1],
            device_id={"gx": west}, device_id_type=MESH),
    ]
    sent = {}

    def send(i, kind, slot, peer):
        place = pieces[i][1](slot)
        copy = pltpu.make_async_remote_copy(
            place, place, send_sem.at[i, kind], recv_sem.at[i, kind],
            device_id={"gy": peer}, device_id_type=MESH)
        copy.start()
        sent[i, kind] = copy

    def give(i):
        if i in staged:
            staged[i].wait()
        else:
            z_copies[i - 4].wait_recv()
        send(i, 0, me, ex)
        send(i, 1, me, wy)
        send(i, 2, me, core)

    def relay(i):
        way = pieces[i][2]
        sent[i, 0].wait_recv()
        if way == 0:
            send(i, 3, ex, wy)
        send(i, 4, ex, core)
        sent[i, 1].wait_recv()
        if way == 1:
            send(i, 3, wy, ex)
        send(i, 5, wy, core)

    def finish(group):
        for i in group:
            sent[i, 3].wait_recv()
            send(i, 6, diag, core)
        for i in group:
            for kind in (2, 4, 5, 6):
                sent[i, kind].wait_recv()

    for i in (0, 1, 2, 3):
        give(i)
    for i in (6, 7):
        staged[i].wait()
    own = lambda ref: ref.at[me]
    pack_edges(levels, own(gd), own(gm), own(gx), own(gt), left, right)
    relay(0)
    for copy in z_copies:
        copy.start()
    relay(1)
    give(4)
    give(5)
    for i in (2, 3, 4, 5):
        relay(i)
    for i in (6, 7):
        send(i, 0, me, ex)
        send(i, 1, me, wy)
        send(i, 2, me, core)
    finish(range(6))

    def readers(j):
        return gathered_block(levels, blocks, codes, j, gd, gm, gx, gt, gel, ger)

    def physics(j, carry):
        there, grid, _, rows = readers(j)
        physics_block(
            levels, width, grid, rows[0], rows[1], there,
            grid_ref, ae.at[j], an.at[j], av.at[j], col.at[j])
        return carry

    lax.fori_loop(0, BPD, physics, 0)
    relay(6)
    relay(7)
    finish((6, 7))

    def advance(j, carry):
        _, _, tracer, rows = readers(j)

        def put(k, value):
            out[k, j] = value

        advance_block(
            levels, width, tracer, rows[2], rows[3], cur,
            ae.at[j], an.at[j], av.at[j], col.at[j], put)
        return carry

    lax.fori_loop(0, BPD, advance, 0)
    for copy in sent.values():
        copy.wait_send()
    for copy in z_copies:
        copy.wait_send()


def run_whole(count, columns, codes, density, sea, mixed, tracer):
    levels, width = density.shape[0], density.shape[-1]
    wide = width + LANES
    hbm = pl.BlockSpec(memory_space=pl.ANY)
    dma = pltpu.SemaphoreType.DMA
    f32 = lambda *shape: pltpu.VMEM(shape, jnp.float32)
    edge = (levels + 1, BPD, LANES)
    many = lambda a: pltpu.VMEM((count,) + a.shape, a.dtype)
    coefficient = f32(BPD, levels, 2 * BR, wide)
    return pl.pallas_call(
        functools.partial(whole_kernel, columns),
        in_specs=[pl.BlockSpec(memory_space=pltpu.SMEM)] + [hbm] * 4,
        out_specs=pl.BlockSpec(memory_space=pltpu.VMEM),
        out_shape=jax.ShapeDtypeStruct(tracer.shape, tracer.dtype),
        scratch_shapes=[
            many(density), many(sea), many(mixed), many(tracer),
            f32(count, *edge), f32(count, *edge), f32(*edge), f32(*edge),
            f32(levels + 2, 3 * BR, wide), f32(levels, 2 * BR, wide),
            coefficient, coefficient, coefficient, f32(BPD, 9, 2 * BR, wide),
            dma((8,)), dma((2,)), dma((2,)), dma((8, 7)), dma((8, 7)),
        ],
        compiler_params=pltpu.CompilerParams(
            collective_id=0, has_side_effects=True, vmem_limit_bytes=60 * 1024 * 1024),
        name="run_whole",
    )(codes, density, sea, mixed, tracer)


def pack_kernel(levels, d, m, x, t, left_ref, right_ref):
    pack_edges(levels, d, m, x, t, left_ref, right_ref)


def block_kernel(levels, width, blocks, codes, *refs):
    d, m, x, t = refs[0:3], refs[3:6], refs[6:9], refs[9:12]
    pel, per, tel, ter = refs[12:15], refs[15:18], refs[18:21], refs[21:24]
    out, grid_ref, cur, ae, an, av, col = refs[24:]
    j = pl.program_id(0)
    code = [codes[3 * j + o] for o in range(3)]
    there = [lax.div(c, blocks * blocks).astype(jnp.float32) for c in code]
    pat = [lax.rem(c, BPD) for c in code]
    dat = [lax.rem(lax.div(c, blocks), BPD) for c in code]

    def grid(o, k):
        if k < levels:
            return d[o][0, k, 0]
        return (m if k == levels else x)[o][0, 0].astype(jnp.float32)

    def row_of(ref, at):
        return lambda o: (lambda r: ref[o][0, r, pl.ds(at[o], 1), :])

    def put(k, value):
        out[k, 0] = value

    physics_block(
        levels, width, grid, row_of(pel, pat), row_of(per, pat), there,
        grid_ref, ae, an, av, col)
    advance_block(
        levels, width, lambda o, k: t[o][0, k, 0], row_of(tel, dat), row_of(ter, dat),
        cur, ae, an, av, col, put)


def run_parts(count, columns, codes, density, sea, mixed, tracer):
    levels, width = density.shape[0], density.shape[-1]
    blocks = count * BPD
    edge = (levels + 1, BPD, LANES)
    shape = jax.ShapeDtypeStruct(edge, jnp.float32)
    left, right = pl.pallas_call(
        functools.partial(pack_kernel, levels), out_shape=[shape, shape], name="pack_edges",
    )(density, sea, mixed, tracer)
    ring = [(i, (i + 1) % columns) for i in range(columns)]
    back = [((i + 1) % columns, i) for i in range(columns)]
    from_west = lax.ppermute(right, "gx", ring)
    from_east = lax.ppermute(left, "gx", back)
    arrays = (density, sea, mixed, tracer, from_west, from_east)
    gd, gm, gx, gt, gel, ger = (lax.all_gather(a, "gy", axis=0) for a in arrays)

    def place(which, j, pre, o):
        code = lax.rem(pre[0][3 * j + o], blocks * blocks)
        slot = lax.div(code, blocks) if which else lax.rem(code, blocks)
        return lax.div(slot, BPD), lax.rem(slot, BPD)

    def five(which, o):
        def at(j, *pre):
            dev, b = place(which, j, pre, o)
            return (dev, 0, b, 0, 0)
        return pl.BlockSpec((1, levels, 1, BR, width), at)

    def four(which, o):
        def at(j, *pre):
            return place(which, j, pre, o) + (0, 0)
        return pl.BlockSpec((1, 1, BR, width), at)

    def edges(which, o):
        def at(j, *pre):
            return (place(which, j, pre, o)[0], 0, 0, 0)
        return pl.BlockSpec((1,) + edge, at)

    three = range(3)
    specs = [five(0, o) for o in three]
    specs += [four(0, o) for o in three] * 2
    specs += [five(1, o) for o in three]
    specs += [edges(0, o) for o in three] * 2
    specs += [edges(1, o) for o in three] * 2
    wide = width + LANES
    f32 = lambda *shape: pltpu.VMEM(shape, jnp.float32)
    return pl.pallas_call(
        functools.partial(block_kernel, levels, width, blocks),
        grid_spec=pltpu.PrefetchScalarGridSpec(
            num_scalar_prefetch=1,
            grid=(BPD,),
            in_specs=specs,
            out_specs=pl.BlockSpec((levels, 1, BR, width), lambda j, *pre: (0, j, 0, 0)),
            scratch_shapes=[f32(levels + 2, 3 * BR, wide)]
            + [f32(levels, 2 * BR, wide)] * 4
            + [f32(9, 2 * BR, wide)],
        ),
        out_shape=jax.ShapeDtypeStruct(tracer.shape, tracer.dtype),
        name="run_blocks",
    )(
        codes,
        gd, gd, gd, gm, gm, gm, gx, gx, gx, gt, gt, gt,
        gel, gel, gel, ger, ger, ger, gel, gel, gel, ger, ger, ger,
    )


def plan(tile_blocks, block_owner):
    blocks = tile_blocks.shape[0]
    at = jnp.arange(blocks, dtype=jnp.int32)
    spot = jnp.arange(3 * BPD, dtype=jnp.int32)
    mine = lax.axis_index("gy") * BPD + spot // 3
    ids = jnp.sum(jnp.where(block_owner[None] == mine[:, None], tile_blocks[None], 0), axis=1)
    near = ids + spot % 3 - 1
    inside = (near >= 0) & (near < blocks)
    hit = tile_blocks[None] == jnp.clip(near, 0, blocks - 1)[:, None]
    codes = jnp.sum(jnp.where(hit, (at + blocks * block_owner)[None], 0), axis=-1)
    return codes + inside.astype(jnp.int32) * (blocks * blocks)


def on_device(count, columns, density, tracer, sea_mask, mixed_level, tile_blocks, block_owner):
    levels, height, width = density.shape
    split = lambda a: a.reshape(a.shape[:-2] + (BPD, BR, width))
    codes = plan(tile_blocks, block_owner)
    density, tracer, sea, mixed = map(split, (density, tracer, sea_mask, mixed_level))
    run = run_whole if count == 8 and columns > 2 else run_parts
    out = run(count, columns, codes, density, sea, mixed, tracer)
    return out.reshape(levels, height, width)


def solution(mesh):
    placed = (P(None, "gy", "gx"), P(None, "gy", "gx"), P("gy", "gx"), P("gy", "gx"), P(), P())
    return jax.shard_map(
        functools.partial(on_device, mesh.shape["gy"], mesh.shape["gx"]),
        mesh=mesh, in_specs=placed, out_specs=P(None, "gy", "gx"), check_vma=False,
    )
```

```python
import functools

import jax
import jax.numpy as jnp
from jax import lax
from jax.experimental import pallas as pl
from jax.experimental.pallas import tpu as pltpu
from jax.sharding import PartitionSpec as P

BR = 8
BPD = 8
ITERS = 4
EDGE = 8
LANES = 128

TIME_STEP = 0.2
STRATIFICATION = 1.0
DENSITY_FLOOR = 0.25
SLOPE_LIMIT = 1.0
TAPER_WIDTH = 0.5
KERNEL_OFFSET = 0.05
BASE_DIFFUSIVITY = 0.2
VISBECK_ALPHA = 0.5

MESH = pl.DeviceIdType.MESH


def own_lane():
    return lax.broadcasted_iota(jnp.int32, (BR, LANES), 1)


def pack_edges(levels, d, m, x, t, left_ref, right_ref, inner):
    lane = own_lane()
    row = lax.broadcasted_iota(jnp.int32, (BR, LANES), 0)
    end = d.shape[-1] - LANES

    def one(tile, shift, keep):
        tile = jnp.where(keep, tile, 0.0)
        tile = pltpu.roll(tile, (shift + (BR - 1) * EDGE) % LANES, 1)
        for bit in (1, 2, 4):
            tile = jnp.where((row & bit) > 0, pltpu.roll(tile, LANES - bit * EDGE, 1), tile)
        return jnp.sum(tile, axis=0, keepdims=True)

    def side(b, start, out_ref, base, keep):
        span = pl.ds(start, LANES)
        tiles = [d[k, b, :, span] for k in range(levels)]
        tiles += [m[b, :, span].astype(jnp.float32), x[b, :, span].astype(jnp.float32)]
        tiles += [t(k, b, start) for k in range(levels)]
        half = LANES // 2
        for j in range(levels + 1):
            out_ref[j, pl.ds(b, 1), :] = (
                one(tiles[2 * j], base, keep) + one(tiles[2 * j + 1], base + half, keep))

    def step(b, carry):
        side(b, 0, left_ref, 0, lane < EDGE)
        side(b, end, right_ref, EDGE, lane >= LANES - EDGE)
        if inner is not None:
            at = (end + LANES) // 2
            tiles = [t(k, b, at) for k in range(levels)]
            for j in range(levels // 2):
                inner[j, pl.ds(b, 1), :] = (
                    one(tiles[2 * j], 0, lane < EDGE)
                    + one(tiles[2 * j + 1], LANES // 2, lane < EDGE))
        return carry

    lax.fori_loop(0, BPD, step, 0)


def spread(row, ch, to):
    base = (ch % 2) * (LANES // 2)
    line = jnp.broadcast_to(row(ch // 2), (BR, LANES))
    shift = (to - base - (BR - 1) * EDGE) % LANES
    return pltpu.roll(line, shift, 1, stride=EDGE, stride_axis=0)


def rim_tile(lane, after, before):
    return jnp.where(lane < EDGE, after, jnp.where(lane >= LANES - EDGE, before, 0.0))


def edge_tile(lane, l_row, r_row, ch):
    return rim_tile(lane, spread(r_row, ch, 0), spread(l_row, ch, LANES - EDGE))


def halves(value, width):
    half = width // 2
    first = lax.broadcasted_iota(jnp.int32, (value.shape[0], LANES), 1) < LANES // 2
    ends = value[:, width:]
    past = jnp.where(first, value[:, half : half + LANES], ends)
    behind = jnp.where(first, ends, value[:, half - LANES : half])
    return (
        jnp.concatenate([value[:, :half], past], axis=1),
        jnp.concatenate([value[:, half:width], behind], axis=1),
    )


def shifts(rows, wide):
    east = lambda f: pltpu.roll(f, wide - 1, 1)
    west = lambda f: pltpu.roll(f, 1, 1)
    north = lambda f: pltpu.roll(f, rows - 1, 0)
    south = lambda f: pltpu.roll(f, 1, 0)
    return east, west, north, south


def physics_block(levels, width, get, l_row, r_row, there, grid_ref, ae_ref, an_ref, av_ref, col, put):
    wide = width + LANES
    rows = 2 * BR
    rim = BR // 2
    lane = own_lane()
    for o in range(3):
        here = pl.ds(o * BR, BR)
        for k in range(levels + 2):
            main = get(o, k)
            tile = edge_tile(lane, l_row(o), r_row(o), k)
            if k == levels:
                main, tile = main * there[o], tile * there[o]
            grid_ref[k, here, :width] = main
            grid_ref[k, here, width:] = tile

    east, west, north, south = shifts(rows, wide)
    mid = lambda k: grid_ref[k, rim : rim + rows, :]
    up = lambda k: grid_ref[k, rim + 1 : rim + 1 + rows, :]
    down = lambda k: grid_ref[k, rim - 1 : rim - 1 + rows, :]

    sea = mid(levels)
    col[0] = sea * east(sea)
    col[1] = sea * west(sea)
    col[2] = sea * up(levels)
    col[3] = sea * down(levels)
    depth = mid(levels + 1)
    col[4] = 1.0 / (depth + 1.0)
    total = jnp.zeros((rows, wide), jnp.float32)
    for k in range(levels):
        c = mid(k)
        ge = 0.5 * ((east(c) - c) * col[0] + (c - west(c)) * col[1])
        gn = 0.5 * ((up(k) - c) * col[2] + (c - down(k)) * col[3])
        hi, lo = min(k + 1, levels - 1), max(k - 1, 0)
        den = jnp.maximum(
            0.5 * (mid(hi) - mid(lo)) + 0.5 * STRATIFICATION * (hi - lo), DENSITY_FLOOR)
        inv = 1.0 / den
        se = -ge * inv
        sn = -gn * inv
        q = se * se + sn * sn
        taper = 0.5 * (1.0 + jnp.tanh((SLOPE_LIMIT - q) * (1.0 / TAPER_WIDTH)))
        factor = taper * jnp.minimum(1.0, (k + 1.0) * col[4]) * mid(levels)
        se = se * factor
        sn = sn * factor
        sq = se * se + sn * sn
        ae_ref[k] = se
        an_ref[k] = sn
        av_ref[k] = sq
        kern = jnp.sqrt(den * (sq + KERNEL_OFFSET))
        total = total + jnp.where(mid(levels + 1) <= k, kern, 0.0)
    sea = mid(levels)
    diff = sea * (
        BASE_DIFFUSIVITY + VISBECK_ALPHA * total / (levels - mid(levels + 1)))
    for k in range(levels):
        put(0, k, ae_ref[k] * diff)
        put(1, k, an_ref[k] * diff)
        put(2, k, av_ref[k] * (0.5 * diff))
    step = (0.5 * TIME_STEP) * sea
    for i in range(4):
        put(3, i, col[i])
    put(3, 4, (diff + east(diff)) * step * col[0])
    put(3, 5, (diff + west(diff)) * step * col[1])
    put(3, 6, (diff + north(diff)) * step * col[2])
    put(3, 7, (diff + south(diff)) * step * col[3])
    put(3, 8, step)


def advance_block(levels, half, get, tile_of, cur, ae_ref, an_ref, av_ref, col, put):
    wide = half + LANES
    rows = 2 * BR
    rim = BR // 2
    for o in range(3):
        first, size, at = ((rim, rim, 0), (0, BR, rim), (0, rim, rim + BR))[o]
        for k in range(levels):
            cur[k, at : at + size, :half] = get(o, k)[first : first + size]
            cur[k, at : at + size, half:] = tile_of(o, k)[first : first + size]
    east, west, north, south = shifts(rows, wide)

    def iterate(_, carry):
        before = None
        flux = None
        held = None
        for k in range(levels):
            c = cur[k]
            de = east(c) - c
            dw = west(de)
            dn = north(c) - c
            ds = south(dn)
            dv = cur[min(k + 1, levels - 1)] - cur[max(k - 1, 0)]
            f = (
                ae_ref[k] * (col[0] * de + col[1] * dw)
                + an_ref[k] * (col[2] * dn + col[3] * ds)
                + av_ref[k] * dv
            )
            u = c + ((col[4] * de - col[5] * dw) + (col[6] * dn - col[7] * ds))
            if k > 0:
                jump = f if before is None else f - before
                cur[k - 1] = held + col[8] * jump
            before, flux, held = flux, f, u
        cur[levels - 1] = held - col[8] * before
        return carry

    lax.fori_loop(0, ITERS, iterate, 0)
    for k in range(levels):
        put(k, cur[k, rim : rim + BR, :half])


def gathered_block(levels, blocks, codes, j, gd, gm, gx, gts, gel, ger, gin):
    code = [codes[3 * j + o] for o in range(3)]
    pair = [lax.rem(c, blocks * blocks) for c in code]
    there = [lax.div(c, blocks * blocks).astype(jnp.float32) for c in code]

    def where(slot):
        return lax.div(slot, BPD), lax.rem(slot, BPD)

    phys = [where(lax.rem(p, blocks)) for p in pair]
    dyn = [where(lax.div(p, blocks)) for p in pair]

    def grid(o, k):
        dev, at = phys[o]
        if k < levels:
            return gd[dev, k, at]
        return (gm if k == levels else gx)[dev, at].astype(jnp.float32)

    def tracer(part):
        def get(o, k):
            dev, at = dyn[o]
            return gts[part][dev, k, at]
        return get

    def row_of(ref, places):
        return lambda o: (lambda r: ref[places[o][0], r, pl.ds(places[o][1], 1), :])

    lane = own_lane()
    l_row, r_row, i_row = (row_of(ref, dyn) for ref in (gel, ger, gin))

    def tile(part):
        def get(o, k):
            ch = levels + 2 + k
            if part == 0:
                after, before = spread(i_row(o), k, 0), spread(l_row(o), ch, LANES - EDGE)
            else:
                dev, at = dyn[o]
                end = gts[0].shape[-1]
                after, before = spread(r_row(o), ch, 0), gts[0][dev, k, at, :, end - LANES :]
            return rim_tile(lane, after, before)
        return get

    return there, grid, row_of(gel, phys), row_of(ger, phys), tracer, tile


def whole_kernel(
    columns, codes, d, m, x, t, out,
    gd, gm, gx, gt0, gt1, gel, ger, gin, left, right,
    grid_ref, cur, raw_e, raw_n, raw_v, raw_c, ae, an, av, col,
    in_sem, z_send, z_recv, send_sem, recv_sem,
):
    levels, width = d.shape[0], d.shape[-1]
    count = gd.shape[0]
    blocks = count * BPD
    me = lax.axis_index("gy")
    mx = lax.axis_index("gx")
    east = lax.rem(mx + 1, columns)
    west = lax.rem(mx + columns - 1, columns)

    def flip(bit):
        return me + bit - 2 * bit * lax.rem(me // bit, 2)

    core, ex, wy = flip(1), flip(2), flip(4)
    diag = flip(2) + flip(4) - me
    low = levels // 2
    cut = lambda ref, h: ref.at[pl.ds(h * low, low)]
    part = lambda ref, h: (lambda slot: ref.at[slot, pl.ds(h * low, low)])
    whole = lambda ref: (lambda slot: ref.at[slot])
    half = width // 2
    side = lambda h, p: t.at[pl.ds(h * low, low), :, :, pl.ds(p * half, half)]
    pieces = [
        (cut(d, 0), part(gd, 0), 0),
        (cut(d, 1), part(gd, 1), 1),
        (m, whole(gm), 0),
        (x, whole(gx), 1),
        (None, whole(gel), 0),
        (None, whole(ger), 1),
        (None, whole(gin), 0),
        (side(0, 0), part(gt0, 0), 0),
        (side(1, 0), part(gt0, 1), 1),
        (side(0, 1), part(gt1, 0), 0),
        (side(1, 1), part(gt1, 1), 1),
    ]
    near, far = (7, 8), (9, 10)
    staged = {}
    for i, (src, place, _) in enumerate(pieces):
        if src is not None:
            staged[i] = pltpu.make_async_copy(src, place(me), in_sem.at[i])
            staged[i].start()

    barrier = pltpu.get_barrier_semaphore()
    for peer in (core, ex, wy):
        pl.semaphore_signal(barrier, inc=1, device_id={"gy": peer}, device_id_type=MESH)
    for peer in (east, west):
        pl.semaphore_signal(barrier, inc=1, device_id={"gx": peer}, device_id_type=MESH)
    pl.semaphore_wait(barrier, 5)

    z_copies = [
        pltpu.make_async_remote_copy(
            right, gel.at[me], z_send.at[0], z_recv.at[0],
            device_id={"gx": east}, device_id_type=MESH),
        pltpu.make_async_remote_copy(
            left, ger.at[me], z_send.at[1], z_recv.at[1],
            device_id={"gx": west}, device_id_type=MESH),
    ]
    sent = {}

    def send(i, kind, slot, peer):
        place = pieces[i][1](slot)
        copy = pltpu.make_async_remote_copy(
            place, place, send_sem.at[i, kind], recv_sem.at[i, kind],
            device_id={"gy": peer}, device_id_type=MESH)
        copy.start()
        sent[i, kind] = copy

    def give(i):
        send(i, 0, me, ex)
        send(i, 1, me, wy)
        send(i, 2, me, core)

    def relay(i):
        way = pieces[i][2]
        sent[i, 0].wait_recv()
        if way == 0:
            send(i, 3, ex, wy)
        send(i, 4, ex, core)
        sent[i, 1].wait_recv()
        if way == 1:
            send(i, 3, wy, ex)
        send(i, 5, wy, core)

    def finish(group):
        for i in group:
            sent[i, 3].wait_recv()
            send(i, 6, diag, core)
        for i in group:
            for kind in (2, 4, 5, 6):
                sent[i, kind].wait_recv()

    for i in (0, 1, 2, 3):
        staged[i].wait()
        give(i)
    for i in near + far:
        staged[i].wait()
    own = lambda ref: ref.at[me]

    def own_tracer(k, b, start):
        ref = gt0 if start < half else gt1
        return ref[me, k, b, :, pl.ds(start % half, LANES)]

    pack_edges(levels, own(gd), own(gm), own(gx), own_tracer, left, right, own(gin))
    relay(0)
    for copy in z_copies:
        copy.start()
    give(6)
    relay(1)
    for i in (4, 5):
        z_copies[i - 4].wait_recv()
        give(i)
    for i in (2, 3, 6, 4, 5):
        relay(i)
    for i in near:
        give(i)
    finish(range(7))

    def readers(j):
        return gathered_block(
            levels, blocks, codes, j, gd, gm, gx, (gt0, gt1), gel, ger, gin)

    def physics(j, carry):
        there, grid, l_row, r_row, _, _ = readers(j)

        def put(which, k, value):
            for p, piece in enumerate(halves(value, width)):
                (ae, an, av, col)[which][p, j, k] = piece

        physics_block(
            levels, width, grid, l_row, r_row, there,
            grid_ref, raw_e, raw_n, raw_v, raw_c, put)
        return carry

    def advance(p):
        def step(j, carry):
            _, _, _, _, tracer, tile = readers(j)

            def put(k, value):
                out[k, j, :, p * half : (p + 1) * half] = value

            advance_block(
                levels, half, tracer(p), tile(p), cur,
                ae.at[p, j], an.at[p, j], av.at[p, j], col.at[p, j], put)
            return carry
        return step

    lax.fori_loop(0, BPD, physics, 0)
    for i in near:
        relay(i)
    for i in far:
        give(i)
    finish(near)
    pause = BPD * 3 // 4
    lax.fori_loop(0, pause, advance(0), 0)
    for i in far:
        relay(i)
    lax.fori_loop(pause, BPD, advance(0), 0)
    finish(far)
    lax.fori_loop(0, BPD, advance(1), 0)
    for copy in sent.values():
        copy.wait_send()
    for copy in z_copies:
        copy.wait_send()


def run_whole(count, columns, codes, density, sea, mixed, tracer):
    levels, width = density.shape[0], density.shape[-1]
    wide = width + LANES
    hbm = pl.BlockSpec(memory_space=pl.ANY)
    dma = pltpu.SemaphoreType.DMA
    f32 = lambda *shape: pltpu.VMEM(shape, jnp.float32)
    edge = (levels + 1, BPD, LANES)
    many = lambda a: pltpu.VMEM((count,) + a.shape, a.dtype)
    slim = width // 2 + LANES
    coefficient = f32(2, BPD, levels, 2 * BR, slim)
    many_half = pltpu.VMEM((count,) + tracer.shape[:-1] + (width // 2,), tracer.dtype)
    return pl.pallas_call(
        functools.partial(whole_kernel, columns),
        in_specs=[pl.BlockSpec(memory_space=pltpu.SMEM)] + [hbm] * 4,
        out_specs=pl.BlockSpec(memory_space=pltpu.VMEM),
        out_shape=jax.ShapeDtypeStruct(tracer.shape, tracer.dtype),
        scratch_shapes=[
            many(density), many(sea), many(mixed), many_half, many_half,
            f32(count, *edge), f32(count, *edge), f32(count, levels // 2, BPD, LANES),
            f32(*edge), f32(*edge),
            f32(levels + 2, 3 * BR, wide), f32(levels, 2 * BR, slim),
            *[f32(levels, 2 * BR, wide)] * 3, f32(5, 2 * BR, wide),
            *[coefficient] * 3, f32(2, BPD, 9, 2 * BR, slim),
            dma((11,)), dma((2,)), dma((2,)), dma((11, 7)), dma((11, 7)),
        ],
        compiler_params=pltpu.CompilerParams(
            collective_id=0, has_side_effects=True, vmem_limit_bytes=60 * 1024 * 1024),
        name="run_whole",
    )(codes, density, sea, mixed, tracer)


def pack_kernel(levels, d, m, x, t, left_ref, right_ref):
    def tracer(k, b, start):
        return t[k, b, :, pl.ds(start, LANES)]

    pack_edges(levels, d, m, x, tracer, left_ref, right_ref, None)


def block_kernel(levels, width, blocks, codes, *refs):
    d, m, x, t = refs[0:3], refs[3:6], refs[6:9], refs[9:12]
    pel, per, tel, ter = refs[12:15], refs[15:18], refs[18:21], refs[21:24]
    out, grid_ref, cur, raw_e, raw_n, raw_v, raw_c, ae, an, av, col = refs[24:]
    j = pl.program_id(0)
    code = [codes[3 * j + o] for o in range(3)]
    there = [lax.div(c, blocks * blocks).astype(jnp.float32) for c in code]
    pat = [lax.rem(c, BPD) for c in code]
    dat = [lax.rem(lax.div(c, blocks), BPD) for c in code]

    def grid(o, k):
        if k < levels:
            return d[o][0, k, 0]
        return (m if k == levels else x)[o][0, 0].astype(jnp.float32)

    def row_of(ref, at):
        return lambda o: (lambda r: ref[o][0, r, pl.ds(at[o], 1), :])

    def put_parts(which, k, value):
        for p, piece in enumerate(halves(value, width)):
            (ae, an, av, col)[which][p, k] = piece

    half = width // 2
    physics_block(
        levels, width, grid, row_of(pel, pat), row_of(per, pat), there,
        grid_ref, raw_e, raw_n, raw_v, raw_c, put_parts)
    lane = own_lane()
    l_row, r_row = row_of(tel, dat), row_of(ter, dat)

    for p in range(2):
        def get(o, k, p=p):
            return t[o][0, k, 0, :, p * half : (p + 1) * half]

        def tile(o, k, p=p):
            ch = levels + 2 + k
            if p == 0:
                after = t[o][0, k, 0, :, half : half + LANES]
                return rim_tile(lane, after, spread(l_row(o), ch, LANES - EDGE))
            before = t[o][0, k, 0, :, half - LANES : half]
            return rim_tile(lane, spread(r_row(o), ch, 0), before)

        def put(k, value, p=p):
            out[k, 0, :, p * half : (p + 1) * half] = value

        advance_block(
            levels, half, get, tile, cur, ae.at[p], an.at[p], av.at[p], col.at[p], put)


def run_parts(count, columns, codes, density, sea, mixed, tracer):
    levels, width = density.shape[0], density.shape[-1]
    blocks = count * BPD
    edge = (levels + 1, BPD, LANES)
    shape = jax.ShapeDtypeStruct(edge, jnp.float32)
    left, right = pl.pallas_call(
        functools.partial(pack_kernel, levels), out_shape=[shape, shape], name="pack_edges",
    )(density, sea, mixed, tracer)
    ring = [(i, (i + 1) % columns) for i in range(columns)]
    back = [((i + 1) % columns, i) for i in range(columns)]
    from_west = lax.ppermute(right, "gx", ring)
    from_east = lax.ppermute(left, "gx", back)
    arrays = (density, sea, mixed, tracer, from_west, from_east)
    gd, gm, gx, gt, gel, ger = (lax.all_gather(a, "gy", axis=0) for a in arrays)

    def place(which, j, pre, o):
        code = lax.rem(pre[0][3 * j + o], blocks * blocks)
        slot = lax.div(code, blocks) if which else lax.rem(code, blocks)
        return lax.div(slot, BPD), lax.rem(slot, BPD)

    def five(which, o):
        def at(j, *pre):
            dev, b = place(which, j, pre, o)
            return (dev, 0, b, 0, 0)
        return pl.BlockSpec((1, levels, 1, BR, width), at)

    def four(which, o):
        def at(j, *pre):
            return place(which, j, pre, o) + (0, 0)
        return pl.BlockSpec((1, 1, BR, width), at)

    def edges(which, o):
        def at(j, *pre):
            return (place(which, j, pre, o)[0], 0, 0, 0)
        return pl.BlockSpec((1,) + edge, at)

    three = range(3)
    slim = width // 2 + LANES
    specs = [five(0, o) for o in three]
    specs += [four(0, o) for o in three] * 2
    specs += [five(1, o) for o in three]
    specs += [edges(0, o) for o in three] * 2
    specs += [edges(1, o) for o in three] * 2
    wide = width + LANES
    f32 = lambda *shape: pltpu.VMEM(shape, jnp.float32)
    return pl.pallas_call(
        functools.partial(block_kernel, levels, width, blocks),
        grid_spec=pltpu.PrefetchScalarGridSpec(
            num_scalar_prefetch=1,
            grid=(BPD,),
            in_specs=specs,
            out_specs=pl.BlockSpec((levels, 1, BR, width), lambda j, *pre: (0, j, 0, 0)),
            scratch_shapes=[f32(levels + 2, 3 * BR, wide), f32(levels, 2 * BR, slim)]
            + [f32(levels, 2 * BR, wide)] * 3
            + [f32(5, 2 * BR, wide)]
            + [f32(2, levels, 2 * BR, slim)] * 3
            + [f32(2, 9, 2 * BR, slim)],
        ),
        out_shape=jax.ShapeDtypeStruct(tracer.shape, tracer.dtype),
        name="run_blocks",
    )(
        codes,
        gd, gd, gd, gm, gm, gm, gx, gx, gx, gt, gt, gt,
        gel, gel, gel, ger, ger, ger, gel, gel, gel, ger, ger, ger,
    )


def plan(tile_blocks, block_owner):
    blocks = tile_blocks.shape[0]
    at = jnp.arange(blocks, dtype=jnp.int32)
    spot = jnp.arange(3 * BPD, dtype=jnp.int32)
    mine = lax.axis_index("gy") * BPD + spot // 3
    ids = jnp.sum(jnp.where(block_owner[None] == mine[:, None], tile_blocks[None], 0), axis=1)
    near = ids + spot % 3 - 1
    inside = (near >= 0) & (near < blocks)
    hit = tile_blocks[None] == jnp.clip(near, 0, blocks - 1)[:, None]
    codes = jnp.sum(jnp.where(hit, (at + blocks * block_owner)[None], 0), axis=-1)
    return codes + inside.astype(jnp.int32) * (blocks * blocks)


def on_device(count, columns, density, tracer, sea_mask, mixed_level, tile_blocks, block_owner):
    levels, height, width = density.shape
    split = lambda a: a.reshape(a.shape[:-2] + (BPD, BR, width))
    codes = plan(tile_blocks, block_owner)
    density, tracer, sea, mixed = map(split, (density, tracer, sea_mask, mixed_level))
    run = run_whole if count == 8 and columns > 2 else run_parts
    out = run(count, columns, codes, density, sea, mixed, tracer)
    return out.reshape(levels, height, width)


def solution(mesh):
    placed = (P(None, "gy", "gx"), P(None, "gy", "gx"), P("gy", "gx"), P("gy", "gx"), P(), P())
    return jax.shard_map(
        functools.partial(on_device, mesh.shape["gy"], mesh.shape["gx"]),
        mesh=mesh, in_specs=placed, out_specs=P(None, "gy", "gx"), check_vma=False,
    )
```

```python
import functools

import jax
import jax.numpy as jnp
from jax import lax
from jax.experimental import pallas as pl
from jax.experimental.pallas import tpu as pltpu
from jax.sharding import PartitionSpec as P

BR = 8
BPD = 8
ITERS = 4
EDGE = 8
LANES = 128

TIME_STEP = 0.2
STRATIFICATION = 1.0
DENSITY_FLOOR = 0.25
SLOPE_LIMIT = 1.0
TAPER_WIDTH = 0.5
KERNEL_OFFSET = 0.05
BASE_DIFFUSIVITY = 0.2
VISBECK_ALPHA = 0.5

MESH = pl.DeviceIdType.MESH


def own_lane():
    return lax.broadcasted_iota(jnp.int32, (BR, LANES), 1)


def pack_edges(levels, d, m, x, t, left_ref, right_ref, inner):
    lane = own_lane()
    row = lax.broadcasted_iota(jnp.int32, (BR, LANES), 0)
    end = d.shape[-1] - LANES

    def one(tile, shift, keep):
        tile = jnp.where(keep, tile, 0.0)
        tile = pltpu.roll(tile, (shift + (BR - 1) * EDGE) % LANES, 1)
        for bit in (1, 2, 4):
            tile = jnp.where((row & bit) > 0, pltpu.roll(tile, LANES - bit * EDGE, 1), tile)
        return jnp.sum(tile, axis=0, keepdims=True)

    def side(b, start, out_ref, base, keep):
        span = pl.ds(start, LANES)
        tiles = [d[k, b, :, span] for k in range(levels)]
        tiles += [m[b, :, span].astype(jnp.float32), x[b, :, span].astype(jnp.float32)]
        tiles += [t(k, b, start) for k in range(levels)]
        half = LANES // 2
        for j in range(levels + 1):
            out_ref[j, pl.ds(b, 1), :] = (
                one(tiles[2 * j], base, keep) + one(tiles[2 * j + 1], base + half, keep))

    def step(b, carry):
        side(b, 0, left_ref, 0, lane < EDGE)
        side(b, end, right_ref, EDGE, lane >= LANES - EDGE)
        if inner is not None:
            at = (end + LANES) // 2
            tiles = [t(k, b, at) for k in range(levels)]
            for j in range(levels // 2):
                inner[j, pl.ds(b, 1), :] = (
                    one(tiles[2 * j], 0, lane < EDGE)
                    + one(tiles[2 * j + 1], LANES // 2, lane < EDGE))
        return carry

    lax.fori_loop(0, BPD, step, 0)


def spread(row, ch, to):
    base = (ch % 2) * (LANES // 2)
    line = jnp.broadcast_to(row(ch // 2), (BR, LANES))
    shift = (to - base - (BR - 1) * EDGE) % LANES
    return pltpu.roll(line, shift, 1, stride=EDGE, stride_axis=0)


def rim_tile(lane, after, before):
    return jnp.where(lane < EDGE, after, jnp.where(lane >= LANES - EDGE, before, 0.0))


def edge_tile(lane, l_row, r_row, ch):
    return rim_tile(lane, spread(r_row, ch, 0), spread(l_row, ch, LANES - EDGE))


def halves(value, width):
    half = width // 2
    first = lax.broadcasted_iota(jnp.int32, (value.shape[0], LANES), 1) < LANES // 2
    ends = value[:, width:]
    past = jnp.where(first, value[:, half : half + LANES], ends)
    behind = jnp.where(first, ends, value[:, half - LANES : half])
    return (
        jnp.concatenate([value[:, :half], past], axis=1),
        jnp.concatenate([value[:, half:width], behind], axis=1),
    )


def shifts(rows, wide):
    east = lambda f: pltpu.roll(f, wide - 1, 1)
    west = lambda f: pltpu.roll(f, 1, 1)
    north = lambda f: pltpu.roll(f, rows - 1, 0)
    south = lambda f: pltpu.roll(f, 1, 0)
    return east, west, north, south


def physics_block(levels, width, get, l_row, r_row, there, grid_ref, ae_ref, an_ref, av_ref, col, put):
    wide = width + LANES
    rows = 2 * BR
    rim = BR // 2
    lane = own_lane()
    for o in range(3):
        here = pl.ds(o * BR, BR)
        for k in range(levels + 2):
            main = get(o, k)
            tile = edge_tile(lane, l_row(o), r_row(o), k)
            if k == levels:
                main, tile = main * there[o], tile * there[o]
            grid_ref[k, here, :width] = main
            grid_ref[k, here, width:] = tile

    east, west, north, south = shifts(rows, wide)
    mid = lambda k: grid_ref[k, rim : rim + rows, :]
    up = lambda k: grid_ref[k, rim + 1 : rim + 1 + rows, :]
    down = lambda k: grid_ref[k, rim - 1 : rim - 1 + rows, :]

    sea = mid(levels)
    col[0] = sea * east(sea)
    col[1] = sea * west(sea)
    col[2] = sea * up(levels)
    col[3] = sea * down(levels)
    depth = mid(levels + 1)
    col[4] = 1.0 / (depth + 1.0)
    total = jnp.zeros((rows, wide), jnp.float32)
    for k in range(levels):
        c = mid(k)
        ge = 0.5 * ((east(c) - c) * col[0] + (c - west(c)) * col[1])
        gn = 0.5 * ((up(k) - c) * col[2] + (c - down(k)) * col[3])
        hi, lo = min(k + 1, levels - 1), max(k - 1, 0)
        den = jnp.maximum(
            0.5 * (mid(hi) - mid(lo)) + 0.5 * STRATIFICATION * (hi - lo), DENSITY_FLOOR)
        inv = 1.0 / den
        se = -ge * inv
        sn = -gn * inv
        q = se * se + sn * sn
        taper = 0.5 * (1.0 + jnp.tanh((SLOPE_LIMIT - q) * (1.0 / TAPER_WIDTH)))
        factor = taper * jnp.minimum(1.0, (k + 1.0) * col[4]) * mid(levels)
        se = se * factor
        sn = sn * factor
        sq = se * se + sn * sn
        ae_ref[k] = se
        an_ref[k] = sn
        av_ref[k] = sq
        kern = jnp.sqrt(den * (sq + KERNEL_OFFSET))
        total = total + jnp.where(mid(levels + 1) <= k, kern, 0.0)
    sea = mid(levels)
    diff = sea * (
        BASE_DIFFUSIVITY + VISBECK_ALPHA * total / (levels - mid(levels + 1)))
    for k in range(levels):
        put(0, k, ae_ref[k] * diff)
        put(1, k, an_ref[k] * diff)
        put(2, k, av_ref[k] * (0.5 * diff))
    step = (0.5 * TIME_STEP) * sea
    for i in range(4):
        put(3, i, col[i])
    put(3, 4, (diff + east(diff)) * step * col[0])
    put(3, 5, (diff + west(diff)) * step * col[1])
    put(3, 6, (diff + north(diff)) * step * col[2])
    put(3, 7, (diff + south(diff)) * step * col[3])
    put(3, 8, step)


def advance_block(levels, half, get, tile_of, cur, ae_ref, an_ref, av_ref, col, put):
    wide = half + LANES
    rows = 2 * BR
    rim = BR // 2
    for o in range(3):
        first, size, at = ((rim, rim, 0), (0, BR, rim), (0, rim, rim + BR))[o]
        for k in range(levels):
            cur[k, at : at + size, :half] = get(o, k)[first : first + size]
            cur[k, at : at + size, half:] = tile_of(o, k)[first : first + size]
    east, west, north, south = shifts(rows, wide)

    def iterate(_, carry):
        before = None
        flux = None
        held = None
        for k in range(levels):
            c = cur[k]
            de = east(c) - c
            dw = west(de)
            dn = north(c) - c
            ds = south(dn)
            dv = cur[min(k + 1, levels - 1)] - cur[max(k - 1, 0)]
            f = (
                ae_ref[k] * (col[0] * de + col[1] * dw)
                + an_ref[k] * (col[2] * dn + col[3] * ds)
                + av_ref[k] * dv
            )
            u = c + ((col[4] * de - col[5] * dw) + (col[6] * dn - col[7] * ds))
            if k > 0:
                jump = f if before is None else f - before
                cur[k - 1] = held + col[8] * jump
            before, flux, held = flux, f, u
        cur[levels - 1] = held - col[8] * before
        return carry

    lax.fori_loop(0, ITERS, iterate, 0)
    for k in range(levels):
        put(k, cur[k, rim : rim + BR, :half])


def gathered_block(levels, blocks, codes, j, gd, gm, gx, gts, gel, ger, gin):
    code = [codes[3 * j + o] for o in range(3)]
    pair = [lax.rem(c, blocks * blocks) for c in code]
    there = [lax.div(c, blocks * blocks).astype(jnp.float32) for c in code]

    def where(slot):
        return lax.div(slot, BPD), lax.rem(slot, BPD)

    phys = [where(lax.rem(p, blocks)) for p in pair]
    dyn = [where(lax.div(p, blocks)) for p in pair]

    def grid(o, k):
        dev, at = phys[o]
        if k < levels:
            return gd[dev, k, at]
        return (gm if k == levels else gx)[dev, at].astype(jnp.float32)

    def tracer(part):
        def get(o, k):
            dev, at = dyn[o]
            return gts[part][dev, k, at]
        return get

    def row_of(ref, places):
        return lambda o: (lambda r: ref[places[o][0], r, pl.ds(places[o][1], 1), :])

    lane = own_lane()
    l_row, r_row, i_row = (row_of(ref, dyn) for ref in (gel, ger, gin))

    def tile(part):
        def get(o, k):
            ch = levels + 2 + k
            if part == 0:
                after, before = spread(i_row(o), k, 0), spread(l_row(o), ch, LANES - EDGE)
            else:
                dev, at = dyn[o]
                end = gts[0].shape[-1]
                after, before = spread(r_row(o), ch, 0), gts[0][dev, k, at, :, end - LANES :]
            return rim_tile(lane, after, before)
        return get

    return there, grid, row_of(gel, phys), row_of(ger, phys), tracer, tile


def whole_kernel(
    columns, codes, d, m, x, t, out,
    gd, gm, gx, gt0, gt1, gel, ger, gin, left, right,
    grid_ref, cur, raw_e, raw_n, raw_v, raw_c, ae, an, av, col,
    in_sem, z_send, z_recv, send_sem, recv_sem,
):
    levels, width = d.shape[0], d.shape[-1]
    count = gd.shape[0]
    blocks = count * BPD
    me = lax.axis_index("gy")
    mx = lax.axis_index("gx")
    east = lax.rem(mx + 1, columns)
    west = lax.rem(mx + columns - 1, columns)

    def flip(bit):
        return me + bit - 2 * bit * lax.rem(me // bit, 2)

    core, ex, wy = flip(1), flip(2), flip(4)
    diag = flip(2) + flip(4) - me
    low = levels // 2
    cut = lambda ref, h: ref.at[pl.ds(h * low, low)]
    part = lambda ref, h: (lambda slot: ref.at[slot, pl.ds(h * low, low)])
    whole = lambda ref: (lambda slot: ref.at[slot])
    half = width // 2
    side = lambda h, p: t.at[pl.ds(h * low, low), :, :, pl.ds(p * half, half)]
    pieces = [
        (cut(d, 0), part(gd, 0), 0),
        (cut(d, 1), part(gd, 1), 1),
        (m, whole(gm), 0),
        (x, whole(gx), 1),
        (None, whole(gel), 0),
        (None, whole(ger), 1),
        (None, whole(gin), 0),
        (side(0, 0), part(gt0, 0), 0),
        (side(1, 0), part(gt0, 1), 1),
        (side(0, 1), part(gt1, 0), 0),
        (side(1, 1), part(gt1, 1), 1),
    ]
    near, far = (7, 8), (9, 10)
    staged = {}
    for i, (src, place, _) in enumerate(pieces):
        if src is not None:
            staged[i] = pltpu.make_async_copy(src, place(me), in_sem.at[i])
            staged[i].start()

    barrier = pltpu.get_barrier_semaphore()
    for peer in (core, ex, wy):
        pl.semaphore_signal(barrier, inc=1, device_id={"gy": peer}, device_id_type=MESH)
    for peer in (east, west):
        pl.semaphore_signal(barrier, inc=1, device_id={"gx": peer}, device_id_type=MESH)
    pl.semaphore_wait(barrier, 5)

    z_copies = [
        pltpu.make_async_remote_copy(
            right, gel.at[me], z_send.at[0], z_recv.at[0],
            device_id={"gx": east}, device_id_type=MESH),
        pltpu.make_async_remote_copy(
            left, ger.at[me], z_send.at[1], z_recv.at[1],
            device_id={"gx": west}, device_id_type=MESH),
    ]
    sent = {}

    def send(i, kind, slot, peer):
        place = pieces[i][1](slot)
        copy = pltpu.make_async_remote_copy(
            place, place, send_sem.at[i, kind], recv_sem.at[i, kind],
            device_id={"gy": peer}, device_id_type=MESH)
        copy.start()
        sent[i, kind] = copy

    def give(i):
        send(i, 0, me, ex)
        send(i, 1, me, wy)
        send(i, 2, me, core)

    def relay(i):
        way = pieces[i][2]
        sent[i, 0].wait_recv()
        if way == 0:
            send(i, 3, ex, wy)
        send(i, 4, ex, core)
        sent[i, 1].wait_recv()
        if way == 1:
            send(i, 3, wy, ex)
        send(i, 5, wy, core)

    def finish(group):
        for i in group:
            sent[i, 3].wait_recv()
            send(i, 6, diag, core)
        for i in group:
            for kind in (2, 4, 5, 6):
                sent[i, kind].wait_recv()

    for i in (0, 1, 2, 3):
        staged[i].wait()
        give(i)
    for i in near + far:
        staged[i].wait()
    own = lambda ref: ref.at[me]

    def own_tracer(k, b, start):
        ref = gt0 if start < half else gt1
        return ref[me, k, b, :, pl.ds(start % half, LANES)]

    pack_edges(levels, own(gd), own(gm), own(gx), own_tracer, left, right, own(gin))
    relay(0)
    for copy in z_copies:
        copy.start()
    give(6)
    relay(1)
    for i in (4, 5):
        z_copies[i - 4].wait_recv()
        give(i)
    for i in (2, 3, 6, 4, 5):
        relay(i)
    for i in near:
        give(i)
    finish(range(7))

    def readers(j):
        return gathered_block(
            levels, blocks, codes, j, gd, gm, gx, (gt0, gt1), gel, ger, gin)

    def physics(j, carry):
        there, grid, l_row, r_row, _, _ = readers(j)

        def put(which, k, value):
            for p, piece in enumerate(halves(value, width)):
                (ae, an, av, col)[which][p, j, k] = piece

        physics_block(
            levels, width, grid, l_row, r_row, there,
            grid_ref, raw_e, raw_n, raw_v, raw_c, put)
        return carry

    def advance(p):
        def step(j, carry):
            _, _, _, _, tracer, tile = readers(j)

            def put(k, value):
                out[k, j, :, p * half : (p + 1) * half] = value

            advance_block(
                levels, half, tracer(p), tile(p), cur,
                ae.at[p, j], an.at[p, j], av.at[p, j], col.at[p, j], put)
            return carry
        return step

    half_way, late = BPD // 2, BPD * 3 // 4
    lax.fori_loop(0, half_way, physics, 0)
    relay(near[0])
    lax.fori_loop(half_way, late, physics, 0)
    relay(near[1])
    for i in far:
        give(i)
    lax.fori_loop(late, BPD, physics, 0)
    finish(near)
    lax.fori_loop(0, half_way, advance(0), 0)
    relay(far[0])
    lax.fori_loop(half_way, late, advance(0), 0)
    relay(far[1])
    lax.fori_loop(late, BPD, advance(0), 0)
    finish(far)
    lax.fori_loop(0, BPD, advance(1), 0)
    for copy in sent.values():
        copy.wait_send()
    for copy in z_copies:
        copy.wait_send()


def run_whole(count, columns, codes, density, sea, mixed, tracer):
    levels, width = density.shape[0], density.shape[-1]
    wide = width + LANES
    hbm = pl.BlockSpec(memory_space=pl.ANY)
    dma = pltpu.SemaphoreType.DMA
    f32 = lambda *shape: pltpu.VMEM(shape, jnp.float32)
    edge = (levels + 1, BPD, LANES)
    many = lambda a: pltpu.VMEM((count,) + a.shape, a.dtype)
    slim = width // 2 + LANES
    coefficient = f32(2, BPD, levels, 2 * BR, slim)
    many_half = pltpu.VMEM((count,) + tracer.shape[:-1] + (width // 2,), tracer.dtype)
    return pl.pallas_call(
        functools.partial(whole_kernel, columns),
        in_specs=[pl.BlockSpec(memory_space=pltpu.SMEM)] + [hbm] * 4,
        out_specs=pl.BlockSpec(memory_space=pltpu.VMEM),
        out_shape=jax.ShapeDtypeStruct(tracer.shape, tracer.dtype),
        scratch_shapes=[
            many(density), many(sea), many(mixed), many_half, many_half,
            f32(count, *edge), f32(count, *edge), f32(count, levels // 2, BPD, LANES),
            f32(*edge), f32(*edge),
            f32(levels + 2, 3 * BR, wide), f32(levels, 2 * BR, slim),
            *[f32(levels, 2 * BR, wide)] * 3, f32(5, 2 * BR, wide),
            *[coefficient] * 3, f32(2, BPD, 9, 2 * BR, slim),
            dma((11,)), dma((2,)), dma((2,)), dma((11, 7)), dma((11, 7)),
        ],
        compiler_params=pltpu.CompilerParams(
            collective_id=0, has_side_effects=True, vmem_limit_bytes=60 * 1024 * 1024),
        name="run_whole",
    )(codes, density, sea, mixed, tracer)


def pack_kernel(levels, d, m, x, t, left_ref, right_ref):
    def tracer(k, b, start):
        return t[k, b, :, pl.ds(start, LANES)]

    pack_edges(levels, d, m, x, tracer, left_ref, right_ref, None)


def block_kernel(levels, width, blocks, codes, *refs):
    d, m, x, t = refs[0:3], refs[3:6], refs[6:9], refs[9:12]
    pel, per, tel, ter = refs[12:15], refs[15:18], refs[18:21], refs[21:24]
    out, grid_ref, cur, raw_e, raw_n, raw_v, raw_c, ae, an, av, col = refs[24:]
    j = pl.program_id(0)
    code = [codes[3 * j + o] for o in range(3)]
    there = [lax.div(c, blocks * blocks).astype(jnp.float32) for c in code]
    pat = [lax.rem(c, BPD) for c in code]
    dat = [lax.rem(lax.div(c, blocks), BPD) for c in code]

    def grid(o, k):
        if k < levels:
            return d[o][0, k, 0]
        return (m if k == levels else x)[o][0, 0].astype(jnp.float32)

    def row_of(ref, at):
        return lambda o: (lambda r: ref[o][0, r, pl.ds(at[o], 1), :])

    def put_parts(which, k, value):
        for p, piece in enumerate(halves(value, width)):
            (ae, an, av, col)[which][p, k] = piece

    half = width // 2
    physics_block(
        levels, width, grid, row_of(pel, pat), row_of(per, pat), there,
        grid_ref, raw_e, raw_n, raw_v, raw_c, put_parts)
    lane = own_lane()
    l_row, r_row = row_of(tel, dat), row_of(ter, dat)

    for p in range(2):
        def get(o, k, p=p):
            return t[o][0, k, 0, :, p * half : (p + 1) * half]

        def tile(o, k, p=p):
            ch = levels + 2 + k
            if p == 0:
                after = t[o][0, k, 0, :, half : half + LANES]
                return rim_tile(lane, after, spread(l_row(o), ch, LANES - EDGE))
            before = t[o][0, k, 0, :, half - LANES : half]
            return rim_tile(lane, spread(r_row(o), ch, 0), before)

        def put(k, value, p=p):
            out[k, 0, :, p * half : (p + 1) * half] = value

        advance_block(
            levels, half, get, tile, cur, ae.at[p], an.at[p], av.at[p], col.at[p], put)


def run_parts(count, columns, codes, density, sea, mixed, tracer):
    levels, width = density.shape[0], density.shape[-1]
    blocks = count * BPD
    edge = (levels + 1, BPD, LANES)
    shape = jax.ShapeDtypeStruct(edge, jnp.float32)
    left, right = pl.pallas_call(
        functools.partial(pack_kernel, levels), out_shape=[shape, shape], name="pack_edges",
    )(density, sea, mixed, tracer)
    ring = [(i, (i + 1) % columns) for i in range(columns)]
    back = [((i + 1) % columns, i) for i in range(columns)]
    from_west = lax.ppermute(right, "gx", ring)
    from_east = lax.ppermute(left, "gx", back)
    arrays = (density, sea, mixed, tracer, from_west, from_east)
    gd, gm, gx, gt, gel, ger = (lax.all_gather(a, "gy", axis=0) for a in arrays)

    def place(which, j, pre, o):
        code = lax.rem(pre[0][3 * j + o], blocks * blocks)
        slot = lax.div(code, blocks) if which else lax.rem(code, blocks)
        return lax.div(slot, BPD), lax.rem(slot, BPD)

    def five(which, o):
        def at(j, *pre):
            dev, b = place(which, j, pre, o)
            return (dev, 0, b, 0, 0)
        return pl.BlockSpec((1, levels, 1, BR, width), at)

    def four(which, o):
        def at(j, *pre):
            return place(which, j, pre, o) + (0, 0)
        return pl.BlockSpec((1, 1, BR, width), at)

    def edges(which, o):
        def at(j, *pre):
            return (place(which, j, pre, o)[0], 0, 0, 0)
        return pl.BlockSpec((1,) + edge, at)

    three = range(3)
    slim = width // 2 + LANES
    specs = [five(0, o) for o in three]
    specs += [four(0, o) for o in three] * 2
    specs += [five(1, o) for o in three]
    specs += [edges(0, o) for o in three] * 2
    specs += [edges(1, o) for o in three] * 2
    wide = width + LANES
    f32 = lambda *shape: pltpu.VMEM(shape, jnp.float32)
    return pl.pallas_call(
        functools.partial(block_kernel, levels, width, blocks),
        grid_spec=pltpu.PrefetchScalarGridSpec(
            num_scalar_prefetch=1,
            grid=(BPD,),
            in_specs=specs,
            out_specs=pl.BlockSpec((levels, 1, BR, width), lambda j, *pre: (0, j, 0, 0)),
            scratch_shapes=[f32(levels + 2, 3 * BR, wide), f32(levels, 2 * BR, slim)]
            + [f32(levels, 2 * BR, wide)] * 3
            + [f32(5, 2 * BR, wide)]
            + [f32(2, levels, 2 * BR, slim)] * 3
            + [f32(2, 9, 2 * BR, slim)],
        ),
        out_shape=jax.ShapeDtypeStruct(tracer.shape, tracer.dtype),
        name="run_blocks",
    )(
        codes,
        gd, gd, gd, gm, gm, gm, gx, gx, gx, gt, gt, gt,
        gel, gel, gel, ger, ger, ger, gel, gel, gel, ger, ger, ger,
    )


def plan(tile_blocks, block_owner):
    blocks = tile_blocks.shape[0]
    at = jnp.arange(blocks, dtype=jnp.int32)
    spot = jnp.arange(3 * BPD, dtype=jnp.int32)
    mine = lax.axis_index("gy") * BPD + spot // 3
    ids = jnp.sum(jnp.where(block_owner[None] == mine[:, None], tile_blocks[None], 0), axis=1)
    near = ids + spot % 3 - 1
    inside = (near >= 0) & (near < blocks)
    hit = tile_blocks[None] == jnp.clip(near, 0, blocks - 1)[:, None]
    codes = jnp.sum(jnp.where(hit, (at + blocks * block_owner)[None], 0), axis=-1)
    return codes + inside.astype(jnp.int32) * (blocks * blocks)


def on_device(count, columns, density, tracer, sea_mask, mixed_level, tile_blocks, block_owner):
    levels, height, width = density.shape
    split = lambda a: a.reshape(a.shape[:-2] + (BPD, BR, width))
    codes = plan(tile_blocks, block_owner)
    density, tracer, sea, mixed = map(split, (density, tracer, sea_mask, mixed_level))
    run = run_whole if count == 8 and columns > 2 else run_parts
    out = run(count, columns, codes, density, sea, mixed, tracer)
    return out.reshape(levels, height, width)


def solution(mesh):
    placed = (P(None, "gy", "gx"), P(None, "gy", "gx"), P("gy", "gx"), P("gy", "gx"), P(), P())
    return jax.shard_map(
        functools.partial(on_device, mesh.shape["gy"], mesh.shape["gx"]),
        mesh=mesh, in_specs=placed, out_specs=P(None, "gy", "gx"), check_vma=False,
    )
```
